32 devices in a mesh: layer: 2 (over y), neuron: 4 (over z), token: 4 (over x, core).
Axes of the slice: x: 2, y: 2, z: 4, core: 2. Of those that a mesh axis runs over, the one named last changes fastest.
Arguments:
- tokens: bfloat16 [4096, 8192], P(('layer', 'token'), 'neuron'), parts along dimension 0, may hold values from -6 to 6
- up_weight: bfloat16 [16384, 14336], P(('layer', 'token'), 'neuron'), parts along dimension 0, may hold values from -0.0625 to 0.0625
- encoder: bfloat16 [16384, 1024], P(('layer', 'token'), 'neuron'), parts along dimension 0, may hold values from -0.0625 to 0.0625
- decoder: bfloat16 [2048, 14336], P(('layer', 'token'), 'neuron'), parts along dimension 0, may hold values from -0.1875 to 0.1875
Outputs:
- grad_encoder: float32 [16384, 1024], P(('layer', 'token'), 'neuron'), parts along dimension 0
- grad_decoder: float32 [2048, 14336], P(('layer', 'token'), 'neuron'), parts along dimension 0
The draws below stay inside these ranges and needn't reach their ends.
There are 2 independent parts, one for each index of `layer`. The reference program is written for one: setup_inputs(seed, part) draws one part's arguments, and reference() takes and returns one part's arrays. A program takes and returns all parts, laid end to end along the dimension named above; each array names one. Nothing has to cross between parts.
All inputs are finite; a program needn't handle non-finite values.
Results may differ from the reference program's by a relative error of at most 0.0034.
Values may be sent and summed in bfloat16 or wider, within the bound.
A program may use at most 128 MiB of HBM per device.

```python
import math
import jax
import jax.numpy as jnp

D = 8192
FF = 14336
RANK = 1024
TOKENS = 2048


def level_of(stream_key, shape, cuts, least, top_value):
    def one(axis_at, parts):
        steps = jax.random.uniform(jax.random.fold_in(jax.random.fold_in(stream_key, 6), axis_at), (parts,), jnp.float32, least / len(cuts), top_value / len(cuts))
        return jnp.repeat(jnp.exp(steps), shape[axis_at] // parts).reshape((-1,) + (1,) * (len(shape) - axis_at - 1))

    factor_of = one(*cuts[0])
    for cut in cuts[1:]:
        factor_of = factor_of * one(*cut)
    return factor_of


def noise(rng, dims, width, bound, shards=(), kind=jnp.bfloat16):
    loudness = level_of(rng, dims, shards, -0.22, 0.18) if shards else 1.0
    drawn = jax.random.normal(rng, dims, jnp.float32) * width * loudness
    return jnp.minimum(jnp.maximum(drawn, -bound), bound).astype(kind)


def setup_inputs(seed: int = 0, part: int = 0) -> dict:
    keys = jax.random.split(jax.random.key(seed), 5)
    own_keys = jax.random.split(jax.random.fold_in(keys[4], part), 5)
    return {
        "tokens": noise(own_keys[0], (TOKENS, D), 1.0, 6.0, ((0, 4), (1, 4))),
        "up_weight": noise(own_keys[1], (D, FF), D ** -0.5, 0.0625, ((0, 4), (1, 4))),
        "encoder": noise(own_keys[2], (D, RANK), D ** -0.5, 0.0625, ((0, 4), (1, 4))),
        "decoder": noise(own_keys[3], (RANK, FF), RANK ** -0.5, 0.1875, ((0, 4), (1, 4))),
    }


def reference(tokens, up_weight, encoder, decoder):
    labels = jax.nn.relu(jnp.dot(tokens, up_weight, preferred_element_type=jnp.float32))
    hidden = jnp.dot(tokens, encoder, preferred_element_type=jnp.float32).astype(jnp.bfloat16)
    predicted = jnp.dot(hidden, decoder, preferred_element_type=jnp.float32)
    scaled = ((predicted - labels) / math.sqrt(TOKENS)).astype(jnp.bfloat16)
    grad_decoder = jnp.dot(hidden.T, scaled, preferred_element_type=jnp.float32)
    back = jnp.dot(scaled, decoder.T, preferred_element_type=jnp.float32).astype(jnp.bfloat16)
    grad_encoder = jnp.dot(tokens.T, back, preferred_element_type=jnp.float32)
    return (grad_encoder, grad_decoder)
```

```python
import math

import jax
import jax.numpy as jnp
from jax import lax
from jax.sharding import PartitionSpec as P

CHUNKS = 4
COLUMN_PARTS = 2


def multiply(left, right):
    return jnp.dot(left, right, preferred_element_type=jnp.float32)


def contract_rows(left, right):
    return lax.dot_general(
        left, right, (((0,), (0,)), ((), ())), preferred_element_type=jnp.float32
    )


def swap(value, axis, offset):
    size = lax.axis_size(axis)
    return lax.ppermute(value, axis, [(i, i ^ offset) for i in range(size)])


def block_at(value, index, width, dim):
    return lax.dynamic_slice_in_dim(value, index * width, width, dim)


def after(value, *earlier):
    return lax.optimization_barrier((value, *earlier))[0]


def reduce_relative(terms_of, axis, wire, trace=None):
    size = lax.axis_size(axis)
    ks = list(range(size))
    held = None
    bit = 1
    while bit < size:
        kept = [k for k in ks if not k & bit]
        sent = [k for k in ks if k & bit]
        if held is None:
            outgoing = terms_of(sent).astype(wire)
            own = terms_of(kept) if trace is None else terms_of(kept, outgoing)
        else:
            outgoing = jnp.stack([held[ks.index(k)] for k in sent]).astype(wire)
            own = jnp.stack([held[ks.index(k)] for k in kept])
        if trace is not None:
            trace.append([outgoing, own])
        held = own + swap(outgoing, axis, bit).astype(jnp.float32)
        ks = kept
        bit *= 2
    if held is None:
        held = terms_of(ks)
    return held[0]


def gather_absolute(value, axis):
    size = lax.axis_size(axis)
    me = lax.axis_index(axis)
    held = value[None]
    order = [0]
    bit = size // 2
    while bit:
        held = jnp.concatenate([held, swap(held, axis, bit)])
        order = order + [k ^ bit for k in order]
        bit //= 2
    place = [order.index(k) for k in range(size)]
    relative = [held[p] for p in place]
    for level in range(size.bit_length() - 1):
        step = 1 << level
        flip = (me & step) != 0
        relative = [
            jnp.where(flip, relative[j ^ step], relative[j]) for j in range(size)
        ]
    return jnp.concatenate(relative)


def per_device(tokens, up_weight, encoder, decoder):
    token_size = lax.axis_size("token")
    neuron_size = lax.axis_size("neuron")
    t = lax.axis_index("token")
    n = lax.axis_index("neuron")
    row_count, width = tokens.shape
    rank_part = encoder.shape[1]
    rank = decoder.shape[0] * token_size
    rank_rows = decoder.shape[0]
    features = width * neuron_size // token_size
    blocks = neuron_size // token_size
    total_rows = row_count * token_size
    chunks = CHUNKS
    rows = row_count // chunks
    scale = 1.0 / math.sqrt(total_rows)

    gathered = [
        lax.all_gather(tokens[c * rows : (c + 1) * rows], "neuron", axis=0, tiled=False)
        for c in range(chunks)
    ]
    decoder_whole = gather_absolute(decoder, "token")

    hiddens, errors, all_pieces = [], [], []
    previous, gates = None, []
    for c in range(chunks):
        source = gathered[c] if previous is None else after(gathered[c], *gates[-1])
        grouped = source.reshape(token_size, blocks, rows, width)

        def features_for(k):
            mine = lax.dynamic_index_in_dim(grouped, t ^ k, 0, keepdims=False)
            return mine.transpose(1, 0, 2).reshape(rows, features)

        pieces = [features_for(0)] + [
            swap(features_for(k), "token", k) for k in range(1, token_size)
        ]
        if previous is not None:
            pieces[1] = after(pieces[1], *previous)

        def terms(ks, weight, earlier=None):
            left = jnp.concatenate([pieces[k] for k in ks])
            if earlier is not None:
                left = after(left, earlier)
            return multiply(left, weight).reshape(len(ks), rows, weight.shape[1])

        label_trace = []
        sums = reduce_relative(
            lambda ks, earlier=None: terms(ks, up_weight, earlier),
            "token",
            jnp.bfloat16,
            label_trace,
        )
        hidden_part = reduce_relative(
            lambda ks: terms(ks, encoder), "token", jnp.float32
        ).astype(jnp.bfloat16)
        others = jnp.stack(
            [hidden_part]
            + [swap(hidden_part, "neuron", m) for m in range(1, neuron_size)]
        )
        hidden = jnp.concatenate(
            [
                lax.dynamic_index_in_dim(others, n ^ j, 0, keepdims=False)
                for j in range(neuron_size)
            ],
            axis=1,
        )
        labels = jax.nn.relu(sums)
        predicted = multiply(hidden, decoder_whole)
        scaled = ((predicted - labels) * scale).astype(jnp.bfloat16)
        previous = label_trace[-1][:1] + errors[-1:]
        gates.append(label_trace[0])
        hiddens.append(hidden)
        errors.append(scaled)
        all_pieces.append(pieces)

    hidden = jnp.concatenate(hiddens)
    scaled = jnp.concatenate(errors)
    columns = scaled.shape[1] // COLUMN_PARTS
    relative = [block_at(hidden, t ^ k, rank_rows, 1) for k in range(token_size)]
    grads = []
    for p in range(COLUMN_PARTS):
        part = scaled[:, p * columns : (p + 1) * columns]

        def grad_terms(ks, part=part):
            left = jnp.concatenate([relative[k] for k in ks], axis=1)
            return contract_rows(left, part).reshape(len(ks), rank_rows, columns)

        grads.append(reduce_relative(grad_terms, "token", jnp.bfloat16))

    back_terms = lax.dot_general(
        scaled, decoder_whole, (((1,), (1,)), ((), ())), preferred_element_type=jnp.float32
    )
    back = block_at(back_terms, n, rank_part, 1)
    for m in range(1, neuron_size):
        outgoing = block_at(back_terms, n ^ m, rank_part, 1).astype(jnp.bfloat16)
        back = back + swap(outgoing, "neuron", m).astype(jnp.float32)
    back = back.astype(jnp.bfloat16)
    backs = [back] + [swap(back, "token", k) for k in range(1, token_size)]
    grad_encoder = contract_rows(
        jnp.concatenate([pieces[k] for k in range(token_size) for pieces in all_pieces]),
        jnp.concatenate(backs),
    )
    return (grad_encoder, jnp.concatenate(grads, axis=1))


def solution(mesh):
    return jax.shard_map(
        per_device,
        mesh=mesh,
        in_specs=(
            P(("layer", "token"), "neuron"),
            P(("layer", "token"), "neuron"),
            P(("layer", "token"), "neuron"),
            P(("layer", "token"), "neuron"),
        ),
        out_specs=(P(("layer", "token"), "neuron"), P(("layer", "token"), "neuron")),
        check_vma=False,
    )
```
